32 devices in a mesh: rows: 16 (over z, y, x), cols: 2 (over core).
Axes of the slice: x: 2, y: 2, z: 4, core: 2. Of those that a mesh axis runs over, the one named last changes fastest.
Arguments:
- panel: float32 [2048, 32768], P('rows', 'cols'), may hold values from -0.03125 to 0.03125
- solved: float32 [32768, 64], P('cols'), may hold values from -6 to 6
- sketch: float32 [2048, 64], P('rows'), may hold values from -6 to 6
- inverses: float32 [2, 1024, 1024], P(None, 'rows', 'cols'), may hold values from -2 to 2, as said below
- coupling: float32 [1024, 1024], P('rows', 'cols'), may hold values from -0.1875 to 0.1875
- design: bfloat16 [32768, 2048], P('rows', 'cols'), may hold values from -0.125 to 0.125
- prior: float32 [32768, 64], P(('rows', 'cols')), may hold values from -6 to 6
Outputs:
- block_solution: float32 [2048, 64], P('rows')
- leverage: float32 [32768], P(('rows', 'cols'))
The draws below stay inside these ranges and needn't reach their ends.
Inputs may be any that keep to these rules, and one draw needn't show every extreme that they name: `inverses`: each of the two blocks is upper triangular with a positive diagonal.
All inputs are finite; a program needn't handle non-finite values.
Results may differ from the reference program's by a relative error of at most 0.00063.
Values sent between devices are 32-bit elements; how exact they have to be, the bound alone decides.
A program may use at most 64 MiB of HBM per device.

```python
import jax
import jax.numpy as jnp
from jax import lax

K = 64
B = 1024
TAIL = 32768
MDEV = 2048
M = 32768
N_ROWS = 16


def draw_inverses(key, part):
    first, second = jax.random.split(jax.random.fold_in(key, 11))
    upper = jnp.clip(jax.random.normal(first, (2, B, B), jnp.float32), -4.0, 4.0)
    upper = upper / jnp.sqrt(jnp.float32(B))
    diagonal = jnp.exp(jax.random.uniform(second, (2, B), jnp.float32, -0.7, 0.4))
    index_row = jax.lax.broadcasted_iota(jnp.int32, (B, B), 0)
    index_col = jax.lax.broadcasted_iota(jnp.int32, (B, B), 1)
    strict = (index_col > index_row).astype(jnp.float32)
    same = (index_col == index_row).astype(jnp.float32)
    return upper * strict[None] + diagonal[:, :, None] * same[None]


def levels(stream_key, dims, shards, low, high):
    gain, own = 1.0, jax.random.fold_in(stream_key, 6)
    for axis_at, parts in shards:
        heights = jnp.exp(jax.random.uniform(jax.random.fold_in(own, axis_at), (parts,), jnp.float32, low / len(shards), high / len(shards)))
        gain = gain * jnp.repeat(heights, dims[axis_at] // parts).reshape([-1 if axis == axis_at else 1 for axis in range(len(dims))])
    return gain


def noise(key, dims, deviation, limit, pieces=(), held_as=jnp.bfloat16):
    values = deviation * jax.random.normal(key, dims, jnp.float32)
    if pieces:
        values = values * levels(key, dims, pieces, -0.22, 0.18)
    return jnp.clip(values, -limit, limit).astype(held_as)


def setup_inputs(seed: int = 0) -> dict:
    key_of = jax.random.split(jax.random.key(seed), 8)
    return {
        "panel": noise(key_of[0], (2 * B, TAIL), TAIL ** -0.5, 0.03125, ((0, 16), (1, 2)), jnp.float32),
        "solved": noise(key_of[1], (TAIL, K), 1.0, 6.0, ((0, 2),), jnp.float32),
        "sketch": noise(key_of[2], (2 * B, K), 1.0, 6.0, ((0, 16),), jnp.float32),
        "inverses": draw_inverses(jax.random.fold_in(key_of[7], 71), 0),
        "coupling": noise(key_of[4], (B, B), B ** -0.5, 0.1875, ((0, 16), (1, 2)), jnp.float32),
        "design": noise(key_of[5], (M, 2 * B), (2 * B) ** -0.5, 0.125, ((0, 16), (1, 2))),
        "prior": noise(key_of[6], (M, K), 1.0, 6.0, ((0, 32),), jnp.float32),
    }


def reference(panel, solved, sketch, inverses, coupling, design, prior):
    highest = lax.Precision.HIGHEST
    right = sketch - jnp.dot(panel, solved, precision=highest)
    y_last = jnp.dot(inverses[1], right[B:], precision=highest)
    bent = jnp.dot(coupling, y_last, precision=highest)
    y_first = jnp.dot(inverses[0], right[:B] - bent, precision=highest)
    block_solution = jnp.concatenate([y_first, y_last], axis=0)
    rounded = block_solution.astype(jnp.bfloat16).astype(jnp.float32)
    stacked = design.reshape(N_ROWS, MDEV, 2 * B)

    def one_block(rows_block):
        return jnp.dot(rows_block.astype(jnp.float32), rounded, precision=highest)

    product = prior + lax.map(one_block, stacked).reshape(N_ROWS * MDEV, K)
    leverage = jnp.mean(product * product, axis=1)
    return block_solution, leverage
```

```python
import functools

import jax
import jax.numpy as jnp
from jax import lax
from jax.experimental import pallas as pl
from jax.experimental.pallas import tpu as pltpu
from jax.sharding import PartitionSpec as P

CHUNKS = 8
NT = (((1,), (1,)), ((), ()))


def nt(a, b, precision=None):
    return lax.dot_general(a, b, NT, precision=precision, preferred_element_type=jnp.float32)


def split(x):
    high = x.astype(jnp.bfloat16)
    low = (x - high.astype(jnp.float32)).astype(jnp.bfloat16)
    return jnp.concatenate([high, low], axis=0)


def kernel(
    n,
    panel, solved, sketch, inverses, coupling, design, prior,
    out_solution, out_leverage,
    panel_v, solved_v, sketch_v, inverses_v, coupling_v, design_v, prior_v,
    acc, part_tx, part_rx, right_tx, right_last, right_first,
    pair_tx, pair_rx, block_tx, gathered, stacked, y_half, sol_tx, sol_rx, prod_tx, prod_rx,
    load_sem, pair_send, pair_recv, send_sem, recv_sem, first_recv, aux_send, aux_recv,
):
    r = lax.axis_index("rows")
    c = lax.axis_index("cols")
    peer = 1 - c
    depth = panel.shape[1]
    step = depth // CHUNKS
    k, pr = sketch.shape
    kh, kq = k // 2, k // 4
    half = n // 2
    quarter = n // 4
    ir = pr // 2

    def chunk(i):
        at = pl.ds(pl.multiple_of(i * step, step), step)
        return (
            pltpu.make_async_copy(panel.at[:, at], panel_v.at[:, at], load_sem.at[0, i]),
            pltpu.make_async_copy(solved.at[:, at], solved_v.at[:, at], load_sem.at[1, i]),
        )

    for i in range(CHUNKS):
        for copy in chunk(i):
            copy.start()
    late = [
        pltpu.make_async_copy(src, dst, load_sem.at[2, i])
        for i, (src, dst) in enumerate(
            (
                (sketch, sketch_v),
                (inverses, inverses_v),
                (coupling, coupling_v),
                (prior, prior_v),
                (design, design_v),
            )
        )
    ]
    for copy in late:
        copy.start()

    barrier = pltpu.get_barrier_semaphore()

    def greet(i, carry):
        pl.semaphore_signal(
            barrier, inc=1, device_id=((r + 1 + i // 2) % n, i % 2), device_id_type=pl.DeviceIdType.MESH
        )
        return carry

    lax.fori_loop(0, 2 * n - 2, greet, 0)
    pl.semaphore_signal(barrier, inc=1, device_id=(r, peer), device_id_type=pl.DeviceIdType.MESH)

    acc[...] = jnp.zeros_like(acc)

    def body(i, carry):
        for copy in chunk(i):
            copy.wait()
        at = pl.ds(pl.multiple_of(i * step, step), step)
        acc[...] += nt(split(solved_v[:, at]), split(panel_v[:, at]))
        return carry

    lax.fori_loop(0, CHUNKS, body, 0)
    total = acc[...]
    part = (total[:k, :pr] + total[k:, :pr]) + (total[:k, pr:] + total[k:, pr:])
    pl.semaphore_wait(barrier, 2 * n - 1)

    def to_peer(src, dst, which):
        return pltpu.make_async_remote_copy(
            src_ref=src,
            dst_ref=dst,
            send_sem=pair_send.at[which],
            recv_sem=pair_recv.at[which],
            device_id=(r, peer),
            device_id_type=pl.DeviceIdType.MESH,
        )

    part_tx[...] = part
    pairs = [to_peer(part_tx.at[pl.ds(pl.multiple_of(kh * peer, kh), kh)], part_rx, 0)]
    pairs[0].start()
    late[0].wait()
    mine = pl.ds(pl.multiple_of(kh * c, kh), kh)
    own = sketch_v[mine, :] - part_tx[mine, :]
    pairs[0].wait_recv()
    right_tx[...] = own - part_rx[...]

    def spread(which, src, dst, core, i, recv):
        to = (r + half + i) % n
        here = jnp.logical_and(to == r, core == c)

        @pl.when(here)
        def _():
            pltpu.make_async_copy(src, dst, recv).start()

        @pl.when(jnp.logical_not(here))
        def _():
            pltpu.make_async_remote_copy(
                src_ref=src,
                dst_ref=dst,
                send_sem=send_sem.at[which, i],
                recv_sem=recv,
                device_id=(to, core),
                device_id_type=pl.DeviceIdType.MESH,
            ).start()

    def settle(which, src, dst, core, i, recv):
        to = (r + half + i) % n
        here = jnp.logical_and(to == r, core == c)

        @pl.when(jnp.logical_not(here))
        def _():
            pltpu.make_async_remote_copy(
                src_ref=src,
                dst_ref=dst,
                send_sem=send_sem.at[which, i],
                recv_sem=recv,
                device_id=(to, core),
                device_id_type=pl.DeviceIdType.MESH,
            ).wait_send()

    def everywhere(act, which, src, dst, core, recv):
        def one(i, carry):
            act(which, src, dst, core, i, recv)
            return carry

        lax.fori_loop(0, n, one, 0)

    last_at = pl.ds(pl.multiple_of(pr * (r % quarter), pr), pr)
    last_args = (0, right_tx, right_last.at[mine, last_at], (r % half) // quarter, recv_sem.at[0])

    def first_rows(act_local, act_remote):
        for i in range(4):
            to, core = (2 * r + i // 2) % n, i % 2
            here = jnp.logical_and(to == r, core == c)

            @pl.when(here)
            def _():
                act_local(pltpu.make_async_copy(right_tx, right_first.at[c], first_recv))

            @pl.when(jnp.logical_not(here))
            def _():
                act_remote(
                    pltpu.make_async_remote_copy(
                        src_ref=right_tx,
                        dst_ref=right_first.at[c],
                        send_sem=send_sem.at[0, i],
                        recv_sem=first_recv,
                        device_id=(to, core),
                        device_id_type=pl.DeviceIdType.MESH,
                    )
                )

    @pl.when(r >= half)
    def _():
        everywhere(spread, *last_args)

    @pl.when(r < half)
    def _():
        first_rows(lambda copy: copy.start(), lambda copy: copy.start())

    def arrived(ref, sem):
        pltpu.make_async_copy(ref, ref, sem).wait()

    lane = lax.broadcasted_iota(jnp.int32, (kh, pr), 1)
    lane_q = lax.broadcasted_iota(jnp.int32, (kq, pr), 1)
    part_at = pl.ds(pl.multiple_of(kq * c, kq), kq)
    peer_at = pl.ds(pl.multiple_of(kq * peer, kq), kq)

    def unfold(a, b):
        low = jnp.where(lane < ir, a, pltpu.roll(b, ir, 1))
        high = jnp.where(lane < ir, pltpu.roll(a, ir, 1), b)
        return jnp.concatenate([low, high], axis=0)

    def pair_sum(operand, weights, which):
        doubled = jnp.concatenate([weights, weights], axis=0)
        whole = nt(operand, doubled, lax.Precision.HIGHEST)
        pair_tx[which] = jnp.where(lane < ir, whole[:kh], whole[kh:])
        copy = to_peer(pair_tx.at[which, peer_at], pair_rx.at[which], which + 1)
        copy.start()
        pairs.append(copy)
        copy.wait_recv()
        return pair_tx[which, part_at, :] + pair_rx[which]

    def load_stacked(which):
        for s in range(quarter):
            a = gathered[which, half * c + 2 * s]
            b = gathered[which, half * c + 2 * s + 1]
            stacked[:, s * pr : (s + 1) * pr] = unfold(a, b)
        return stacked[...]

    def block_args(which, core):
        return (
            which + 1,
            block_tx.at[which],
            gathered.at[which, r, part_at],
            core,
            recv_sem.at[which + 1],
        )

    side = r // half
    half_at = pl.ds(pl.multiple_of(half * c, half), half)

    late[1].wait()
    arrived(right_last, recv_sem.at[0])
    block_tx[0] = pair_sum(right_last[...], inverses_v[1], 0)
    everywhere(spread, *block_args(0, side))
    late[2].wait()
    arrived(gathered.at[0, half_at], recv_sem.at[1])

    def handover():
        return pltpu.make_async_remote_copy(
            src_ref=gathered.at[0, pl.ds(0, half)],
            dst_ref=gathered.at[0, pl.ds(0, half)],
            send_sem=aux_send.at[0],
            recv_sem=aux_recv.at[0],
            device_id=(r, peer),
            device_id_type=pl.DeviceIdType.MESH,
        )

    @pl.when(c == 0)
    def _():
        handover().start()

    bent = pair_sum(load_stacked(0), coupling_v[...], 1)
    arrived(right_first, first_recv)
    a, b = right_first[0, part_at, :], right_first[1, part_at, :]
    even = jnp.where(lane_q < ir, a, pltpu.roll(b, ir, 1))
    odd = jnp.where(lane_q < ir, pltpu.roll(a, ir, 1), b)
    block_tx[1] = jnp.where(r % 2 == 0, even, odd) - bent
    everywhere(spread, *block_args(1, side))
    arrived(gathered.at[1, half_at], recv_sem.at[2])

    block_tx[2] = pair_sum(load_stacked(1), inverses_v[0], 2)
    everywhere(spread, *block_args(2, 0))
    late[3].wait()
    late[4].wait()

    sol_copy = pltpu.make_async_remote_copy(
        src_ref=sol_tx,
        dst_ref=sol_rx,
        send_sem=aux_send.at[1],
        recv_sem=aux_recv.at[1],
        device_id=(r, peer),
        device_id_type=pl.DeviceIdType.MESH,
    )

    def finish(which):
        for s in range(half):
            both = unfold(gathered[which, 2 * s], gathered[which, 2 * s + 1])
            y_half[:, s * pr : (s + 1) * pr] = both.astype(jnp.bfloat16)
        at = 2 * (r % half)

        @pl.when(side == c)
        def _():
            both = unfold(gathered[which, at], gathered[which, at + 1])
            sol_tx[...] = both
            sol_copy.start()
            out_solution[...] = both

    @pl.when(c == 0)
    def _():
        arrived(gathered.at[2], recv_sem.at[3])
        finish(2)

    @pl.when(c == 1)
    def _():
        handover().wait_recv()
        finish(0)

    rows_here = prior.shape[1]

    def product(which):
        at = pl.ds(pl.multiple_of(rows_here * which, rows_here), rows_here)
        return nt(y_half[...], design_v[at, :])

    prod_copy = pltpu.make_async_remote_copy(
        src_ref=prod_tx,
        dst_ref=prod_rx,
        send_sem=aux_send.at[2],
        recv_sem=aux_recv.at[2],
        device_id=(r, peer),
        device_id_type=pl.DeviceIdType.MESH,
    )
    prod_tx[...] = product(peer)
    prod_copy.start()
    held = product(c) + prior_v[...]
    prod_copy.wait_recv()
    whole = held + prod_rx[...]
    out_leverage[...] = jnp.mean(whole * whole, axis=0, keepdims=True)

    @pl.when(side != c)
    def _():
        sol_copy.wait_recv()
        out_solution[...] = sol_rx[...]

    @pl.when(side == c)
    def _():
        sol_copy.wait_send()

    prod_copy.wait_send()

    @pl.when(c == 0)
    def _():
        handover().wait_send()

    for copy in pairs:
        copy.wait_send()

    @pl.when(r >= half)
    def _():
        everywhere(settle, *last_args)

    @pl.when(r < half)
    def _():
        first_rows(lambda copy: None, lambda copy: copy.wait_send())

    for which, core in ((0, side), (1, side), (2, 0)):
        everywhere(settle, *block_args(which, core))


def fused(n, panel, solved, sketch, inverses, coupling, design, prior):
    k = sketch.shape[1]
    pr, depth = panel.shape
    rows_here = prior.shape[0]
    width = inverses.shape[2]
    kh, kq = k // 2, k // 4
    f32 = jnp.float32
    out_solution, out_leverage = pl.pallas_call(
        functools.partial(kernel, n),
        out_shape=(
            jax.ShapeDtypeStruct((k, pr), f32),
            jax.ShapeDtypeStruct((1, rows_here), f32),
        ),
        in_specs=[pl.BlockSpec(memory_space=pl.ANY)] * 7,
        out_specs=[pl.BlockSpec(memory_space=pltpu.VMEM)] * 2,
        scratch_shapes=[
            pltpu.VMEM((pr, depth), f32),
            pltpu.VMEM((k, depth), f32),
            pltpu.VMEM((k, pr), f32),
            pltpu.VMEM(inverses.shape, f32),
            pltpu.VMEM(coupling.shape, f32),
            pltpu.VMEM(design.shape, design.dtype),
            pltpu.VMEM((k, rows_here), f32),
            pltpu.VMEM((2 * k, 2 * pr), f32),
            pltpu.VMEM((k, pr), f32),
            pltpu.VMEM((kh, pr), f32),
            pltpu.VMEM((kh, pr), f32),
            pltpu.VMEM((k, width), f32),
            pltpu.VMEM((2, kh, pr), f32),
            pltpu.VMEM((3, kh, pr), f32),
            pltpu.VMEM((3, kq, pr), f32),
            pltpu.VMEM((3, kq, pr), f32),
            pltpu.VMEM((3, n, kh, pr), f32),
            pltpu.VMEM((k, width), f32),
            pltpu.VMEM((k, 2 * width), jnp.bfloat16),
            pltpu.VMEM((k, pr), f32),
            pltpu.VMEM((k, pr), f32),
            pltpu.VMEM((k, rows_here), f32),
            pltpu.VMEM((k, rows_here), f32),
            pltpu.SemaphoreType.DMA((3, CHUNKS)),
            pltpu.SemaphoreType.DMA((4,)),
            pltpu.SemaphoreType.DMA((4,)),
            pltpu.SemaphoreType.DMA((4, n)),
            pltpu.SemaphoreType.DMA((4,)),
            pltpu.SemaphoreType.DMA,
            pltpu.SemaphoreType.DMA((3,)),
            pltpu.SemaphoreType.DMA((3,)),
        ],
        compiler_params=pltpu.CompilerParams(
            collective_id=0, has_side_effects=True, vmem_limit_bytes=48 * 1024 * 1024
        ),
    )(panel, solved.T, sketch.T, inverses, coupling, design, prior.T)
    return out_solution.T, out_leverage.reshape(rows_here)


def assemble(term):
    rows_here = lax.psum(term, "cols")
    return lax.all_gather(rows_here, "rows", axis=0, tiled=True)


def local(panel, solved, sketch, inverses, coupling, design, prior):
    highest = lax.Precision.HIGHEST
    partial_value = jnp.dot(panel, solved, precision=highest)
    local_right = sketch - lax.psum(partial_value, "cols")
    right = lax.all_gather(local_right, "rows", axis=0, tiled=True)
    blocks = right.shape[0] // 2
    width = inverses.shape[2]
    column = lax.axis_index("cols")
    offset = column * width

    def piece(vector):
        return lax.dynamic_slice_in_dim(vector, offset, width, 0)

    right_first = right[:blocks]
    right_last = right[blocks:]
    sketch_cols = right.shape[1]
    inverse_full = lax.all_gather(inverses[0], "cols", axis=1, tiled=True)
    coupling_full = lax.all_gather(coupling, "rows", axis=0, tiled=True)
    mixed = jnp.dot(inverse_full, coupling_full, precision=highest)
    term_last = jnp.dot(inverses[1], piece(right_last), precision=highest)
    term_first = jnp.dot(inverses[0], piece(right_first), precision=highest)
    joined = assemble(jnp.concatenate([term_last, term_first], axis=1))
    y_last = joined[:, :sketch_cols]
    partial_first = joined[:, sketch_cols:]
    correction = assemble(jnp.dot(mixed, piece(y_last), precision=highest))
    y_first = partial_first - correction
    solution = jnp.concatenate([y_first, y_last], axis=0)
    own_rows = sketch.shape[0]
    block_solution = lax.dynamic_slice_in_dim(
        solution, lax.axis_index("rows") * own_rows, own_rows, 0
    )
    design_cols = design.shape[1]
    rounded = lax.dynamic_slice_in_dim(solution, column * design_cols, design_cols, 0).astype(
        jnp.bfloat16
    )
    mine = lax.psum_scatter(
        jnp.dot(design, rounded, preferred_element_type=jnp.float32),
        "cols",
        scatter_dimension=0,
        tiled=True,
    )
    product = prior + mine
    leverage = jnp.mean(product * product, axis=1)
    return (block_solution, leverage)


def local_or_fused(rows, panel, solved, sketch, inverses, coupling, design, prior):
    args = (panel, solved, sketch, inverses, coupling, design, prior)
    pr, depth = panel.shape
    fits = pr == 128 and depth % (CHUNKS * 128) == 0 and sketch.shape[1] % 32 == 0
    return fused(rows, *args) if fits else local(*args)


def solution(mesh):
    in_specs = (
        P("rows", "cols"),
        P("cols", None),
        P("rows", None),
        P(None, "rows", "cols"),
        P("rows", "cols"),
        P("rows", "cols"),
        P(("rows", "cols"), None),
    )
    out_specs = (P("rows", None), P(("rows", "cols")))
    rows, cols = mesh.shape["rows"], mesh.shape["cols"]
    step = local
    if cols == 2 and rows % 4 == 0:
        step = functools.partial(local_or_fused, rows)
    return jax.shard_map(step, mesh=mesh, in_specs=in_specs, out_specs=out_specs, check_vma=False)
```

```python
import functools

import jax
import jax.numpy as jnp
from jax import lax
from jax.experimental import pallas as pl
from jax.experimental.pallas import tpu as pltpu
from jax.sharding import PartitionSpec as P

CHUNKS = 8
NT = (((1,), (1,)), ((), ()))


def nt(a, b, precision=None):
    return lax.dot_general(a, b, NT, precision=precision, preferred_element_type=jnp.float32)


def split(x):
    high = x.astype(jnp.bfloat16)
    low = (x - high.astype(jnp.float32)).astype(jnp.bfloat16)
    return jnp.concatenate([high, low], axis=0)


def kernel(
    n,
    panel, solved, sketch, inverses, coupling, design, prior,
    out_solution, out_leverage,
    panel_v, solved_v, sketch_v, inverses_v, coupling_v, design_v, prior_v,
    acc, part_tx, part_rx, right_tx, right_last, right_first,
    pair_tx, pair_rx, block_tx, gathered, stacked, y_half, sol_tx, sol_rx, prod_tx, prod_rx, split_v,
    load_sem, pair_send, pair_recv, send_sem, recv_sem, first_recv, aux_send, aux_recv,
):
    r = lax.axis_index("rows")
    c = lax.axis_index("cols")
    peer = 1 - c
    depth = panel.shape[1]
    step = depth // CHUNKS
    k, pr = sketch.shape
    kh, kq = k // 2, k // 4
    half = n // 2
    quarter = n // 4
    ir = pr // 2

    def chunk(i):
        at = pl.ds(pl.multiple_of(i * step, step), step)
        return (
            pltpu.make_async_copy(panel.at[:, at], panel_v.at[:, at], load_sem.at[0, i]),
            pltpu.make_async_copy(solved.at[:, at], solved_v.at[:, at], load_sem.at[1, i]),
        )

    for i in range(CHUNKS):
        for copy in chunk(i):
            copy.start()
    late = [
        pltpu.make_async_copy(src, dst, load_sem.at[2, i])
        for i, (src, dst) in enumerate(
            (
                (sketch, sketch_v),
                (inverses, inverses_v),
                (coupling, coupling_v),
                (prior, prior_v),
                (design, design_v),
            )
        )
    ]
    for copy in late:
        copy.start()

    barrier = pltpu.get_barrier_semaphore()

    def greet(i, carry):
        pl.semaphore_signal(
            barrier, inc=1, device_id=((r + 1 + i // 2) % n, i % 2), device_id_type=pl.DeviceIdType.MESH
        )
        return carry

    lax.fori_loop(0, 2 * n - 2, greet, 0)
    pl.semaphore_signal(barrier, inc=1, device_id=(r, peer), device_id_type=pl.DeviceIdType.MESH)

    acc[...] = jnp.zeros_like(acc)

    def body(i, carry):
        for copy in chunk(i):
            copy.wait()
        at = pl.ds(pl.multiple_of(i * step, step), step)
        acc[...] += nt(split(solved_v[:, at]), split(panel_v[:, at]))
        return carry

    lax.fori_loop(0, CHUNKS, body, 0)
    total = acc[...]
    part = (total[:k, :pr] + total[k:, :pr]) + (total[:k, pr:] + total[k:, pr:])
    pl.semaphore_wait(barrier, 2 * n - 1)

    def to_peer(src, dst, which):
        return pltpu.make_async_remote_copy(
            src_ref=src,
            dst_ref=dst,
            send_sem=pair_send.at[which],
            recv_sem=pair_recv.at[which],
            device_id=(r, peer),
            device_id_type=pl.DeviceIdType.MESH,
        )

    part_tx[...] = part
    pairs = [to_peer(part_tx.at[pl.ds(pl.multiple_of(kh * peer, kh), kh)], part_rx, 0)]
    pairs[0].start()
    late[0].wait()
    mine = pl.ds(pl.multiple_of(kh * c, kh), kh)
    own = sketch_v[mine, :] - part_tx[mine, :]
    pairs[0].wait_recv()
    right_tx[...] = own - part_rx[...]

    def spread(which, src, dst, core, i, recv):
        to = (r + half + i) % n
        here = jnp.logical_and(to == r, core == c)

        @pl.when(here)
        def _():
            pltpu.make_async_copy(src, dst, recv).start()

        @pl.when(jnp.logical_not(here))
        def _():
            pltpu.make_async_remote_copy(
                src_ref=src,
                dst_ref=dst,
                send_sem=send_sem.at[which, i],
                recv_sem=recv,
                device_id=(to, core),
                device_id_type=pl.DeviceIdType.MESH,
            ).start()

    def settle(which, src, dst, core, i, recv):
        to = (r + half + i) % n
        here = jnp.logical_and(to == r, core == c)

        @pl.when(jnp.logical_not(here))
        def _():
            pltpu.make_async_remote_copy(
                src_ref=src,
                dst_ref=dst,
                send_sem=send_sem.at[which, i],
                recv_sem=recv,
                device_id=(to, core),
                device_id_type=pl.DeviceIdType.MESH,
            ).wait_send()

    def everywhere(act, which, src, dst, core, recv):
        def one(i, carry):
            act(which, src, dst, core, i, recv)
            return carry

        lax.fori_loop(0, n, one, 0)

    last_at = pl.ds(pl.multiple_of(pr * (r % quarter), pr), pr)
    last_args = (0, right_tx, right_last.at[mine, last_at], (r % half) // quarter, recv_sem.at[0])

    def first_rows(act_local, act_remote):
        for i in range(4):
            to, core = (2 * r + i // 2) % n, i % 2
            here = jnp.logical_and(to == r, core == c)

            @pl.when(here)
            def _():
                act_local(pltpu.make_async_copy(right_tx, right_first.at[c], first_recv))

            @pl.when(jnp.logical_not(here))
            def _():
                act_remote(
                    pltpu.make_async_remote_copy(
                        src_ref=right_tx,
                        dst_ref=right_first.at[c],
                        send_sem=send_sem.at[0, i],
                        recv_sem=first_recv,
                        device_id=(to, core),
                        device_id_type=pl.DeviceIdType.MESH,
                    )
                )

    @pl.when(r >= half)
    def _():
        everywhere(spread, *last_args)

    @pl.when(r < half)
    def _():
        first_rows(lambda copy: copy.start(), lambda copy: copy.start())

    def arrived(ref, sem):
        pltpu.make_async_copy(ref, ref, sem).wait()

    lane = lax.broadcasted_iota(jnp.int32, (kh, pr), 1)
    lane_q = lax.broadcasted_iota(jnp.int32, (kq, pr), 1)
    part_at = pl.ds(pl.multiple_of(kq * c, kq), kq)
    peer_at = pl.ds(pl.multiple_of(kq * peer, kq), kq)

    def unfold(a, b):
        low = jnp.where(lane < ir, a, pltpu.roll(b, ir, 1))
        high = jnp.where(lane < ir, pltpu.roll(a, ir, 1), b)
        return jnp.concatenate([low, high], axis=0)

    def pair_sum(operand, weights, which):
        terms = nt(split(operand), weights)
        terms = terms[:k] + terms[k:]
        whole = terms[:, :pr] + terms[:, pr:]
        pair_tx[which] = jnp.where(lane < ir, whole[:kh], whole[kh:])
        copy = to_peer(pair_tx.at[which, peer_at], pair_rx.at[which], which + 1)
        copy.start()
        pairs.append(copy)
        copy.wait_recv()
        return pair_tx[which, part_at, :] + pair_rx[which]

    def load_stacked(which):
        for s in range(quarter):
            a = gathered[which, half * c + 2 * s]
            b = gathered[which, half * c + 2 * s + 1]
            stacked[:, s * pr : (s + 1) * pr] = unfold(a, b)
        return stacked[...]

    def block_args(which, core):
        return (
            which + 1,
            block_tx.at[which],
            gathered.at[which, r, part_at],
            core,
            recv_sem.at[which + 1],
        )

    side = r // half
    half_at = pl.ds(pl.multiple_of(half * c, half), half)

    late[1].wait()
    late[2].wait()
    for i, weights in enumerate((inverses_v[1], coupling_v[...], inverses_v[0])):
        split_v[i] = split(jnp.concatenate([weights, weights], axis=0))

    arrived(right_last, recv_sem.at[0])
    block_tx[0] = pair_sum(right_last[...], split_v[0], 0)
    everywhere(spread, *block_args(0, side))
    arrived(gathered.at[0, half_at], recv_sem.at[1])

    def handover():
        return pltpu.make_async_remote_copy(
            src_ref=gathered.at[0, pl.ds(0, half)],
            dst_ref=gathered.at[0, pl.ds(0, half)],
            send_sem=aux_send.at[0],
            recv_sem=aux_recv.at[0],
            device_id=(r, peer),
            device_id_type=pl.DeviceIdType.MESH,
        )

    @pl.when(c == 0)
    def _():
        handover().start()

    bent = pair_sum(load_stacked(0), split_v[1], 1)
    arrived(right_first, first_recv)
    a, b = right_first[0, part_at, :], right_first[1, part_at, :]
    even = jnp.where(lane_q < ir, a, pltpu.roll(b, ir, 1))
    odd = jnp.where(lane_q < ir, pltpu.roll(a, ir, 1), b)
    block_tx[1] = jnp.where(r % 2 == 0, even, odd) - bent
    everywhere(spread, *block_args(1, side))
    arrived(gathered.at[1, half_at], recv_sem.at[2])

    block_tx[2] = pair_sum(load_stacked(1), split_v[2], 2)
    everywhere(spread, *block_args(2, 0))
    late[3].wait()
    late[4].wait()

    sol_copy = pltpu.make_async_remote_copy(
        src_ref=sol_tx,
        dst_ref=sol_rx,
        send_sem=aux_send.at[1],
        recv_sem=aux_recv.at[1],
        device_id=(r, peer),
        device_id_type=pl.DeviceIdType.MESH,
    )

    def finish(which):
        for s in range(half):
            both = unfold(gathered[which, 2 * s], gathered[which, 2 * s + 1])
            y_half[:, s * pr : (s + 1) * pr] = both.astype(jnp.bfloat16)
        at = 2 * (r % half)

        @pl.when(side == c)
        def _():
            both = unfold(gathered[which, at], gathered[which, at + 1])
            sol_tx[...] = both
            sol_copy.start()
            out_solution[...] = both

    @pl.when(c == 0)
    def _():
        arrived(gathered.at[2], recv_sem.at[3])
        finish(2)

    @pl.when(c == 1)
    def _():
        handover().wait_recv()
        finish(0)

    rows_here = prior.shape[1]

    def product(which):
        at = pl.ds(pl.multiple_of(rows_here * which, rows_here), rows_here)
        return nt(y_half[...], design_v[at, :])

    prod_copy = pltpu.make_async_remote_copy(
        src_ref=prod_tx,
        dst_ref=prod_rx,
        send_sem=aux_send.at[2],
        recv_sem=aux_recv.at[2],
        device_id=(r, peer),
        device_id_type=pl.DeviceIdType.MESH,
    )
    prod_tx[...] = product(peer)
    prod_copy.start()
    held = product(c) + prior_v[...]
    prod_copy.wait_recv()
    whole = held + prod_rx[...]
    out_leverage[...] = jnp.mean(whole * whole, axis=0, keepdims=True)

    @pl.when(side != c)
    def _():
        sol_copy.wait_recv()
        out_solution[...] = sol_rx[...]

    @pl.when(side == c)
    def _():
        sol_copy.wait_send()

    prod_copy.wait_send()

    @pl.when(c == 0)
    def _():
        handover().wait_send()

    for copy in pairs:
        copy.wait_send()

    @pl.when(r >= half)
    def _():
        everywhere(settle, *last_args)

    @pl.when(r < half)
    def _():
        first_rows(lambda copy: None, lambda copy: copy.wait_send())

    for which, core in ((0, side), (1, side), (2, 0)):
        everywhere(settle, *block_args(which, core))


def fused(n, panel, solved, sketch, inverses, coupling, design, prior):
    k = sketch.shape[1]
    pr, depth = panel.shape
    rows_here = prior.shape[0]
    width = inverses.shape[2]
    kh, kq = k // 2, k // 4
    f32 = jnp.float32
    out_solution, out_leverage = pl.pallas_call(
        functools.partial(kernel, n),
        out_shape=(
            jax.ShapeDtypeStruct((k, pr), f32),
            jax.ShapeDtypeStruct((1, rows_here), f32),
        ),
        in_specs=[pl.BlockSpec(memory_space=pl.ANY)] * 7,
        out_specs=[pl.BlockSpec(memory_space=pltpu.VMEM)] * 2,
        scratch_shapes=[
            pltpu.VMEM((pr, depth), f32),
            pltpu.VMEM((k, depth), f32),
            pltpu.VMEM((k, pr), f32),
            pltpu.VMEM(inverses.shape, f32),
            pltpu.VMEM(coupling.shape, f32),
            pltpu.VMEM(design.shape, design.dtype),
            pltpu.VMEM((k, rows_here), f32),
            pltpu.VMEM((2 * k, 2 * pr), f32),
            pltpu.VMEM((k, pr), f32),
            pltpu.VMEM((kh, pr), f32),
            pltpu.VMEM((kh, pr), f32),
            pltpu.VMEM((k, width), f32),
            pltpu.VMEM((2, kh, pr), f32),
            pltpu.VMEM((3, kh, pr), f32),
            pltpu.VMEM((3, kq, pr), f32),
            pltpu.VMEM((3, kq, pr), f32),
            pltpu.VMEM((3, n, kh, pr), f32),
            pltpu.VMEM((k, width), f32),
            pltpu.VMEM((k, 2 * width), jnp.bfloat16),
            pltpu.VMEM((k, pr), f32),
            pltpu.VMEM((k, pr), f32),
            pltpu.VMEM((k, rows_here), f32),
            pltpu.VMEM((k, rows_here), f32),
            pltpu.VMEM((3, 2 * pr, width), jnp.bfloat16),
            pltpu.SemaphoreType.DMA((3, CHUNKS)),
            pltpu.SemaphoreType.DMA((4,)),
            pltpu.SemaphoreType.DMA((4,)),
            pltpu.SemaphoreType.DMA((4, n)),
            pltpu.SemaphoreType.DMA((4,)),
            pltpu.SemaphoreType.DMA,
            pltpu.SemaphoreType.DMA((3,)),
            pltpu.SemaphoreType.DMA((3,)),
        ],
        compiler_params=pltpu.CompilerParams(
            collective_id=0, has_side_effects=True, vmem_limit_bytes=60 * 1024 * 1024
        ),
    )(panel, solved.T, sketch.T, inverses, coupling, design, prior.T)
    return out_solution.T, out_leverage.reshape(rows_here)


def assemble(term):
    rows_here = lax.psum(term, "cols")
    return lax.all_gather(rows_here, "rows", axis=0, tiled=True)


def local(panel, solved, sketch, inverses, coupling, design, prior):
    highest = lax.Precision.HIGHEST
    partial_value = jnp.dot(panel, solved, precision=highest)
    local_right = sketch - lax.psum(partial_value, "cols")
    right = lax.all_gather(local_right, "rows", axis=0, tiled=True)
    blocks = right.shape[0] // 2
    width = inverses.shape[2]
    column = lax.axis_index("cols")
    offset = column * width

    def piece(vector):
        return lax.dynamic_slice_in_dim(vector, offset, width, 0)

    right_first = right[:blocks]
    right_last = right[blocks:]
    sketch_cols = right.shape[1]
    inverse_full = lax.all_gather(inverses[0], "cols", axis=1, tiled=True)
    coupling_full = lax.all_gather(coupling, "rows", axis=0, tiled=True)
    mixed = jnp.dot(inverse_full, coupling_full, precision=highest)
    term_last = jnp.dot(inverses[1], piece(right_last), precision=highest)
    term_first = jnp.dot(inverses[0], piece(right_first), precision=highest)
    joined = assemble(jnp.concatenate([term_last, term_first], axis=1))
    y_last = joined[:, :sketch_cols]
    partial_first = joined[:, sketch_cols:]
    correction = assemble(jnp.dot(mixed, piece(y_last), precision=highest))
    y_first = partial_first - correction
    solution = jnp.concatenate([y_first, y_last], axis=0)
    own_rows = sketch.shape[0]
    block_solution = lax.dynamic_slice_in_dim(
        solution, lax.axis_index("rows") * own_rows, own_rows, 0
    )
    design_cols = design.shape[1]
    rounded = lax.dynamic_slice_in_dim(solution, column * design_cols, design_cols, 0).astype(
        jnp.bfloat16
    )
    mine = lax.psum_scatter(
        jnp.dot(design, rounded, preferred_element_type=jnp.float32),
        "cols",
        scatter_dimension=0,
        tiled=True,
    )
    product = prior + mine
    leverage = jnp.mean(product * product, axis=1)
    return (block_solution, leverage)


def local_or_fused(rows, panel, solved, sketch, inverses, coupling, design, prior):
    args = (panel, solved, sketch, inverses, coupling, design, prior)
    pr, depth = panel.shape
    fits = pr == 128 and depth % (CHUNKS * 128) == 0 and sketch.shape[1] % 32 == 0
    return fused(rows, *args) if fits else local(*args)


def solution(mesh):
    in_specs = (
        P("rows", "cols"),
        P("cols", None),
        P("rows", None),
        P(None, "rows", "cols"),
        P("rows", "cols"),
        P("rows", "cols"),
        P(("rows", "cols"), None),
    )
    out_specs = (P("rows", None), P(("rows", "cols")))
    rows, cols = mesh.shape["rows"], mesh.shape["cols"]
    step = local
    if cols == 2 and rows % 4 == 0:
        step = functools.partial(local_or_fused, rows)
    return jax.shard_map(step, mesh=mesh, in_specs=in_specs, out_specs=out_specs, check_vma=False)
```

```python
import functools

import jax
import jax.numpy as jnp
from jax import lax
from jax.experimental import pallas as pl
from jax.experimental.pallas import tpu as pltpu
from jax.sharding import PartitionSpec as P

CHUNKS = 8
NT = (((1,), (1,)), ((), ()))


def nt(a, b, precision=None):
    return lax.dot_general(a, b, NT, precision=precision, preferred_element_type=jnp.float32)


def split(x):
    high = x.astype(jnp.bfloat16)
    low = (x - high.astype(jnp.float32)).astype(jnp.bfloat16)
    return jnp.concatenate([high, low], axis=0)


def kernel(
    n,
    panel, solved, sketch, inverses, coupling, design, prior,
    out_solution, out_leverage,
    panel_v, solved_v, sketch_v, inverses_v, coupling_v, design_v, prior_v,
    acc, part_tx, part_rx, right_tx, right_last, right_first,
    pair_tx, pair_rx, block_tx, gathered, stacked, y_half, sol_tx, sol_rx, prod_tx, prod_rx, split_v,
    load_sem, pair_send, pair_recv, send_sem, recv_sem, first_recv, aux_send, aux_recv,
    cross_sem,
):
    r = lax.axis_index("rows")
    c = lax.axis_index("cols")
    peer = 1 - c
    depth = panel.shape[1]
    step = depth // CHUNKS
    k, pr = sketch.shape
    kh, kq = k // 2, k // 4
    half = n // 2
    quarter = n // 4
    ir = pr // 2

    def chunk(i):
        at = pl.ds(pl.multiple_of(i * step, step), step)
        return (
            pltpu.make_async_copy(panel.at[:, at], panel_v.at[:, at], load_sem.at[0, i]),
            pltpu.make_async_copy(solved.at[:, at], solved_v.at[:, at], load_sem.at[1, i]),
        )

    for i in range(CHUNKS):
        for copy in chunk(i):
            copy.start()
    late = [
        pltpu.make_async_copy(src, dst, load_sem.at[2, i])
        for i, (src, dst) in enumerate(
            (
                (sketch, sketch_v),
                (inverses, inverses_v),
                (coupling, coupling_v),
                (prior, prior_v),
                (design, design_v),
            )
        )
    ]
    for copy in late:
        copy.start()

    barrier = pltpu.get_barrier_semaphore()

    def greet(i, carry):
        pl.semaphore_signal(
            barrier, inc=1, device_id=((r + 1 + i // 2) % n, i % 2), device_id_type=pl.DeviceIdType.MESH
        )
        return carry

    lax.fori_loop(0, 2 * n - 2, greet, 0)
    pl.semaphore_signal(barrier, inc=1, device_id=(r, peer), device_id_type=pl.DeviceIdType.MESH)

    acc[...] = jnp.zeros_like(acc)

    def body(i, carry):
        for copy in chunk(i):
            copy.wait()
        at = pl.ds(pl.multiple_of(i * step, step), step)
        acc[...] += nt(split(solved_v[:, at]), split(panel_v[:, at]))
        return carry

    lax.fori_loop(0, CHUNKS, body, 0)
    total = acc[...]
    part = (total[:k, :pr] + total[k:, :pr]) + (total[:k, pr:] + total[k:, pr:])
    pl.semaphore_wait(barrier, 2 * n - 1)

    def to_peer(src, dst, which):
        return pltpu.make_async_remote_copy(
            src_ref=src,
            dst_ref=dst,
            send_sem=pair_send.at[which],
            recv_sem=pair_recv.at[which],
            device_id=(r, peer),
            device_id_type=pl.DeviceIdType.MESH,
        )

    part_tx[...] = part
    pairs = [to_peer(part_tx.at[pl.ds(pl.multiple_of(kh * peer, kh), kh)], part_rx, 0)]
    pairs[0].start()
    late[0].wait()
    mine = pl.ds(pl.multiple_of(kh * c, kh), kh)
    own = sketch_v[mine, :] - part_tx[mine, :]
    pairs[0].wait_recv()
    right_tx[...] = own - part_rx[...]

    side = r // half
    other = (r + half) % n

    def target(i):
        return half * side + (r % half + i) % half

    def across(which, src, dst, core):
        return pltpu.make_async_remote_copy(
            src_ref=src,
            dst_ref=dst,
            send_sem=send_sem.at[which, half],
            recv_sem=cross_sem.at[which],
            device_id=(other, core),
            device_id_type=pl.DeviceIdType.MESH,
        )

    def relay(which, ref, act):
        def one(i, carry):
            act(
                pltpu.make_async_remote_copy(
                    src_ref=ref,
                    dst_ref=ref,
                    send_sem=send_sem.at[which, half + i],
                    recv_sem=recv_sem.at[which],
                    device_id=(target(i), c),
                    device_id_type=pl.DeviceIdType.MESH,
                )
            )
            return carry

        lax.fori_loop(1, half, one, 0)

    def spread(which, src, dst, core, i, recv):
        to = target(i)
        here = jnp.logical_and(to == r, core == c)

        @pl.when(here)
        def _():
            pltpu.make_async_copy(src, dst, recv).start()

        @pl.when(jnp.logical_not(here))
        def _():
            pltpu.make_async_remote_copy(
                src_ref=src,
                dst_ref=dst,
                send_sem=send_sem.at[which, i],
                recv_sem=recv,
                device_id=(to, core),
                device_id_type=pl.DeviceIdType.MESH,
            ).start()

    def settle(which, src, dst, core, i, recv):
        to = target(i)
        here = jnp.logical_and(to == r, core == c)

        @pl.when(jnp.logical_not(here))
        def _():
            pltpu.make_async_remote_copy(
                src_ref=src,
                dst_ref=dst,
                send_sem=send_sem.at[which, i],
                recv_sem=recv,
                device_id=(to, core),
                device_id_type=pl.DeviceIdType.MESH,
            ).wait_send()

    def everywhere(act, which, src, dst, core, recv):
        def one(i, carry):
            act(which, src, dst, core, i, recv)
            return carry

        lax.fori_loop(0, half, one, 0)

    last_at = pl.ds(pl.multiple_of(pr * (r % quarter), pr), pr)
    last_args = (0, right_tx, right_last.at[mine, last_at], (r % half) // quarter, recv_sem.at[0])

    def first_rows(act_local, act_remote):
        for i in range(4):
            to, core = (2 * r + i // 2) % n, i % 2
            here = jnp.logical_and(to == r, core == c)

            @pl.when(here)
            def _():
                act_local(pltpu.make_async_copy(right_tx, right_first.at[c], first_recv))

            @pl.when(jnp.logical_not(here))
            def _():
                act_remote(
                    pltpu.make_async_remote_copy(
                        src_ref=right_tx,
                        dst_ref=right_first.at[c],
                        send_sem=send_sem.at[4, i],
                        recv_sem=first_recv,
                        device_id=(to, core),
                        device_id_type=pl.DeviceIdType.MESH,
                    )
                )

    @pl.when(r >= half)
    def _():
        across(*last_args[:4]).start()
        everywhere(spread, *last_args)

    @pl.when(r < half)
    def _():
        first_rows(lambda copy: copy.start(), lambda copy: copy.start())

    def arrived(ref, sem):
        pltpu.make_async_copy(ref, ref, sem).wait()

    relays_last = jnp.logical_and(r < half, c == (r % half) // quarter)
    last_ref = right_last.at[:, last_at]

    def blocks_in(which):
        @pl.when(c == side)
        def _():
            arrived(gathered.at[which, half_at], recv_sem.at[which + 1])

        @pl.when(c != side)
        def _():
            arrived(gathered.at[which, other], cross_sem.at[which + 1])
            relay(which + 1, gathered.at[which, other], lambda copy: copy.start())
            arrived(gathered.at[which, pl.ds(0, half - 1)], recv_sem.at[which + 1])

    lane = lax.broadcasted_iota(jnp.int32, (kh, pr), 1)
    lane_q = lax.broadcasted_iota(jnp.int32, (kq, pr), 1)
    part_at = pl.ds(pl.multiple_of(kq * c, kq), kq)
    peer_at = pl.ds(pl.multiple_of(kq * peer, kq), kq)

    def unfold(a, b):
        low = jnp.where(lane < ir, a, pltpu.roll(b, ir, 1))
        high = jnp.where(lane < ir, pltpu.roll(a, ir, 1), b)
        return jnp.concatenate([low, high], axis=0)

    def pair_sum(operand, weights, which):
        terms = nt(split(operand), weights)
        terms = terms[:k] + terms[k:]
        whole = terms[:, :pr] + terms[:, pr:]
        pair_tx[which] = jnp.where(lane < ir, whole[:kh], whole[kh:])
        copy = to_peer(pair_tx.at[which, peer_at], pair_rx.at[which], which + 1)
        copy.start()
        pairs.append(copy)
        copy.wait_recv()
        return pair_tx[which, part_at, :] + pair_rx[which]

    def load_stacked(which):
        for s in range(quarter):
            a = gathered[which, half * c + 2 * s]
            b = gathered[which, half * c + 2 * s + 1]
            stacked[:, s * pr : (s + 1) * pr] = unfold(a, b)
        return stacked[...]

    def block_args(which, core):
        return (
            which + 1,
            block_tx.at[which],
            gathered.at[which, r, part_at],
            core,
            recv_sem.at[which + 1],
        )

    half_at = pl.ds(pl.multiple_of(half * c, half), half)

    late[1].wait()
    late[2].wait()
    for i, weights in enumerate((inverses_v[1], coupling_v[...], inverses_v[0])):
        split_v[i] = split(jnp.concatenate([weights, weights], axis=0))

    @pl.when(relays_last)
    def _():
        arrived(last_ref, cross_sem.at[0])
        relay(0, last_ref, lambda copy: copy.start())
        arrived(right_last.at[:, pl.ds(0, right_last.shape[1] - pr)], recv_sem.at[0])

    @pl.when(jnp.logical_not(relays_last))
    def _():
        arrived(right_last, recv_sem.at[0])

    block_tx[0] = pair_sum(right_last[...], split_v[0], 0)
    across(*block_args(0, side)[:4]).start()
    everywhere(spread, *block_args(0, side))
    blocks_in(0)

    def handover():
        return pltpu.make_async_remote_copy(
            src_ref=gathered.at[0, pl.ds(0, half)],
            dst_ref=gathered.at[0, pl.ds(0, half)],
            send_sem=aux_send.at[0],
            recv_sem=aux_recv.at[0],
            device_id=(r, peer),
            device_id_type=pl.DeviceIdType.MESH,
        )

    @pl.when(c == 0)
    def _():
        handover().start()

    bent = pair_sum(load_stacked(0), split_v[1], 1)
    arrived(right_first, first_recv)
    a, b = right_first[0, part_at, :], right_first[1, part_at, :]
    even = jnp.where(lane_q < ir, a, pltpu.roll(b, ir, 1))
    odd = jnp.where(lane_q < ir, pltpu.roll(a, ir, 1), b)
    block_tx[1] = jnp.where(r % 2 == 0, even, odd) - bent
    across(*block_args(1, side)[:4]).start()
    everywhere(spread, *block_args(1, side))
    blocks_in(1)

    block_tx[2] = pair_sum(load_stacked(1), split_v[2], 2)
    across(*block_args(2, 0)[:4]).start()
    everywhere(spread, *block_args(2, 0))
    late[3].wait()
    late[4].wait()

    sol_copy = pltpu.make_async_remote_copy(
        src_ref=sol_tx,
        dst_ref=sol_rx,
        send_sem=aux_send.at[1],
        recv_sem=aux_recv.at[1],
        device_id=(r, peer),
        device_id_type=pl.DeviceIdType.MESH,
    )

    def finish(which):
        for s in range(half):
            both = unfold(gathered[which, 2 * s], gathered[which, 2 * s + 1])
            y_half[:, s * pr : (s + 1) * pr] = both.astype(jnp.bfloat16)
        at = 2 * (r % half)

        @pl.when(side == c)
        def _():
            both = unfold(gathered[which, at], gathered[which, at + 1])
            sol_tx[...] = both
            sol_copy.start()
            out_solution[...] = both

    @pl.when(c == 0)
    def _():
        arrived(gathered.at[2, other], cross_sem.at[3])
        relay(3, gathered.at[2, other], lambda copy: copy.start())
        arrived(gathered.at[2, pl.ds(0, n - 1)], recv_sem.at[3])
        finish(2)

    @pl.when(c == 1)
    def _():
        handover().wait_recv()
        finish(0)

    rows_here = prior.shape[1]

    def product(which):
        at = pl.ds(pl.multiple_of(rows_here * which, rows_here), rows_here)
        return nt(y_half[...], design_v[at, :])

    prod_copy = pltpu.make_async_remote_copy(
        src_ref=prod_tx,
        dst_ref=prod_rx,
        send_sem=aux_send.at[2],
        recv_sem=aux_recv.at[2],
        device_id=(r, peer),
        device_id_type=pl.DeviceIdType.MESH,
    )
    prod_tx[...] = product(peer)
    prod_copy.start()
    held = product(c) + prior_v[...]
    prod_copy.wait_recv()
    whole = held + prod_rx[...]
    out_leverage[...] = jnp.mean(whole * whole, axis=0, keepdims=True)

    @pl.when(side != c)
    def _():
        sol_copy.wait_recv()
        out_solution[...] = sol_rx[...]

    @pl.when(side == c)
    def _():
        sol_copy.wait_send()

    prod_copy.wait_send()

    @pl.when(c == 0)
    def _():
        handover().wait_send()

    for copy in pairs:
        copy.wait_send()

    @pl.when(r >= half)
    def _():
        across(*last_args[:4]).wait_send()
        everywhere(settle, *last_args)

    @pl.when(relays_last)
    def _():
        relay(0, last_ref, lambda copy: copy.wait_send())

    @pl.when(r < half)
    def _():
        first_rows(lambda copy: None, lambda copy: copy.wait_send())

    for which, core in ((0, side), (1, side), (2, 0)):
        across(*block_args(which, core)[:4]).wait_send()
        everywhere(settle, *block_args(which, core))

    @pl.when(c != side)
    def _():
        for which in (0, 1):
            relay(which + 1, gathered.at[which, other], lambda copy: copy.wait_send())

    @pl.when(c == 0)
    def _():
        relay(3, gathered.at[2, other], lambda copy: copy.wait_send())


def fused(n, panel, solved, sketch, inverses, coupling, design, prior):
    k = sketch.shape[1]
    pr, depth = panel.shape
    rows_here = prior.shape[0]
    width = inverses.shape[2]
    kh, kq = k // 2, k // 4
    f32 = jnp.float32
    out_solution, out_leverage = pl.pallas_call(
        functools.partial(kernel, n),
        out_shape=(
            jax.ShapeDtypeStruct((k, pr), f32),
            jax.ShapeDtypeStruct((1, rows_here), f32),
        ),
        in_specs=[pl.BlockSpec(memory_space=pl.ANY)] * 7,
        out_specs=[pl.BlockSpec(memory_space=pltpu.VMEM)] * 2,
        scratch_shapes=[
            pltpu.VMEM((pr, depth), f32),
            pltpu.VMEM((k, depth), f32),
            pltpu.VMEM((k, pr), f32),
            pltpu.VMEM(inverses.shape, f32),
            pltpu.VMEM(coupling.shape, f32),
            pltpu.VMEM(design.shape, design.dtype),
            pltpu.VMEM((k, rows_here), f32),
            pltpu.VMEM((2 * k, 2 * pr), f32),
            pltpu.VMEM((k, pr), f32),
            pltpu.VMEM((kh, pr), f32),
            pltpu.VMEM((kh, pr), f32),
            pltpu.VMEM((k, width), f32),
            pltpu.VMEM((2, kh, pr), f32),
            pltpu.VMEM((3, kh, pr), f32),
            pltpu.VMEM((3, kq, pr), f32),
            pltpu.VMEM((3, kq, pr), f32),
            pltpu.VMEM((3, n, kh, pr), f32),
            pltpu.VMEM((k, width), f32),
            pltpu.VMEM((k, 2 * width), jnp.bfloat16),
            pltpu.VMEM((k, pr), f32),
            pltpu.VMEM((k, pr), f32),
            pltpu.VMEM((k, rows_here), f32),
            pltpu.VMEM((k, rows_here), f32),
            pltpu.VMEM((3, 2 * pr, width), jnp.bfloat16),
            pltpu.SemaphoreType.DMA((3, CHUNKS)),
            pltpu.SemaphoreType.DMA((4,)),
            pltpu.SemaphoreType.DMA((4,)),
            pltpu.SemaphoreType.DMA((5, n)),
            pltpu.SemaphoreType.DMA((4,)),
            pltpu.SemaphoreType.DMA,
            pltpu.SemaphoreType.DMA((3,)),
            pltpu.SemaphoreType.DMA((3,)),
            pltpu.SemaphoreType.DMA((4,)),
        ],
        compiler_params=pltpu.CompilerParams(
            collective_id=0, has_side_effects=True, vmem_limit_bytes=60 * 1024 * 1024
        ),
    )(panel, solved.T, sketch.T, inverses, coupling, design, prior.T)
    return out_solution.T, out_leverage.reshape(rows_here)


def assemble(term):
    rows_here = lax.psum(term, "cols")
    return lax.all_gather(rows_here, "rows", axis=0, tiled=True)


def local(panel, solved, sketch, inverses, coupling, design, prior):
    highest = lax.Precision.HIGHEST
    partial_value = jnp.dot(panel, solved, precision=highest)
    local_right = sketch - lax.psum(partial_value, "cols")
    right = lax.all_gather(local_right, "rows", axis=0, tiled=True)
    blocks = right.shape[0] // 2
    width = inverses.shape[2]
    column = lax.axis_index("cols")
    offset = column * width

    def piece(vector):
        return lax.dynamic_slice_in_dim(vector, offset, width, 0)

    right_first = right[:blocks]
    right_last = right[blocks:]
    sketch_cols = right.shape[1]
    inverse_full = lax.all_gather(inverses[0], "cols", axis=1, tiled=True)
    coupling_full = lax.all_gather(coupling, "rows", axis=0, tiled=True)
    mixed = jnp.dot(inverse_full, coupling_full, precision=highest)
    term_last = jnp.dot(inverses[1], piece(right_last), precision=highest)
    term_first = jnp.dot(inverses[0], piece(right_first), precision=highest)
    joined = assemble(jnp.concatenate([term_last, term_first], axis=1))
    y_last = joined[:, :sketch_cols]
    partial_first = joined[:, sketch_cols:]
    correction = assemble(jnp.dot(mixed, piece(y_last), precision=highest))
    y_first = partial_first - correction
    solution = jnp.concatenate([y_first, y_last], axis=0)
    own_rows = sketch.shape[0]
    block_solution = lax.dynamic_slice_in_dim(
        solution, lax.axis_index("rows") * own_rows, own_rows, 0
    )
    design_cols = design.shape[1]
    rounded = lax.dynamic_slice_in_dim(solution, column * design_cols, design_cols, 0).astype(
        jnp.bfloat16
    )
    mine = lax.psum_scatter(
        jnp.dot(design, rounded, preferred_element_type=jnp.float32),
        "cols",
        scatter_dimension=0,
        tiled=True,
    )
    product = prior + mine
    leverage = jnp.mean(product * product, axis=1)
    return (block_solution, leverage)


def local_or_fused(rows, panel, solved, sketch, inverses, coupling, design, prior):
    args = (panel, solved, sketch, inverses, coupling, design, prior)
    pr, depth = panel.shape
    fits = pr == 128 and depth % (CHUNKS * 128) == 0 and sketch.shape[1] % 32 == 0
    return fused(rows, *args) if fits else local(*args)


def solution(mesh):
    in_specs = (
        P("rows", "cols"),
        P("cols", None),
        P("rows", None),
        P(None, "rows", "cols"),
        P("rows", "cols"),
        P("rows", "cols"),
        P(("rows", "cols"), None),
    )
    out_specs = (P("rows", None), P(("rows", "cols")))
    rows, cols = mesh.shape["rows"], mesh.shape["cols"]
    step = local
    if cols == 2 and rows % 4 == 0:
        step = functools.partial(local_or_fused, rows)
    return jax.shard_map(step, mesh=mesh, in_specs=in_specs, out_specs=out_specs, check_vma=False)
```
